32 devices in a mesh: graph: 8 (over z, x), batch: 4 (over y, core).
Axes of the slice: x: 2, y: 2, z: 4, core: 2. Of those that a mesh axis runs over, the one named last changes fastest.
Arguments:
- node_latent: bfloat16 [4, 1024, 512], P('batch', 'graph'), may hold values from -6 to 6
- edge_latent: bfloat16 [4, 8192, 512], P('batch', 'graph'), may hold values from -6 to 6
- node_cotangent: bfloat16 [4, 1024, 512], P('batch', 'graph'), may hold values from -6 to 6
- edge_w_in: bfloat16 [2, 1536, 512], replicated, may hold values from -0.15625 to 0.15625
- edge_w_out: bfloat16 [2, 512, 512], replicated, may hold values from -0.25 to 0.25
- node_w_in: bfloat16 [2, 1024, 512], replicated, may hold values from -0.1875 to 0.1875
- node_w_out: bfloat16 [2, 512, 512], replicated, may hold values from -0.25 to 0.25
- edge_gain: float32 [2, 512], replicated, may hold values from 0.25 to 1.75
- node_gain: float32 [2, 512], replicated, may hold values from 0.25 to 1.75
- edge_slot: int32 [8192], P('graph'), may hold values from 0 to 383, as said below
- edge_receiver: int32 [8192], P('graph'), may hold values from 0 to 127
- send_list: int32 [64, 32], P('graph'), may hold values from 0 to 127, as said below
- edge_count: int32 [8], P('graph'), may hold values from 256 to 1024, as said below
Outputs:
- node_out: float32 [4, 1024, 512], P('batch', 'graph')
- node_grad: float32 [4, 1024, 512], P('batch', 'graph')
- grad_edge_in: float32 [2, 1536, 512], P(None, ('graph', 'batch'))
- grad_edge_out: float32 [2, 512, 512], P(None, ('graph', 'batch'))
- grad_node_in: float32 [2, 1024, 512], P(None, ('graph', 'batch'))
- grad_node_out: float32 [2, 512, 512], P(None, ('graph', 'batch'))
- grad_edge_gain: float32 [2, 512], P(None, ('graph', 'batch'))
- grad_node_gain: float32 [2, 512], P(None, ('graph', 'batch'))
The draws below stay inside these ranges and needn't reach their ends.
Inputs may be any that keep to these rules, and one draw needn't show every extreme that they name: `edge_slot`: for edge j of partition p = j // 1024: a slot below 128 names a node of partition p; a slot s of 128 or more names row (s - 128) % 32 of the list that partition q = (s - 128) // 32 keeps for partition p, and q differs from p cyclically by 1 to 2 steps or by exactly 8 // 2 steps. `edge_receiver`: the receiving node is a node of the edge's own partition. `send_list`: row q * 8 + p holds 32 distinct node numbers within partition q, the nodes whose latents partition p may read. `edge_count`: edge slots at or above a partition's count carry no edge.
All inputs are finite; a program needn't handle non-finite values.
Results may differ from the reference program's by a relative error of at most 0.035.
Values may be sent and summed in bfloat16 or wider, within the bound.
A program may use at most 128 MiB of HBM per device.

```python
import jax
import jax.numpy as jnp
from jax import lax

D = 512
HID = 512
LAYERS = 2
HOPS = 2
NOD_DEV = 128
EDGE_CAP = 1024
PEER_CAP = 32
NODES = 1024
EDGES = 8192
SAMPLES = 4
N_GRAPH = 8


def draw_edge_slot(key, part):
    subkeys = jax.random.split(jax.random.fold_in(key, 11), 4)
    edge_ids = jnp.arange(EDGES, dtype=jnp.int32)
    owner = edge_ids // EDGE_CAP
    is_local = jax.random.randint(subkeys[0], (EDGES,), 0, 2) == 0
    local_slot = jax.random.randint(subkeys[1], (EDGES,), 0, NOD_DEV)
    hop_pick = jax.random.randint(subkeys[2], (EDGES,), 0, 2 * HOPS + 1)
    offset = jnp.where(hop_pick < HOPS, hop_pick - HOPS, jnp.where(hop_pick < 2 * HOPS, hop_pick - HOPS + 1, N_GRAPH // 2))
    source = (owner + offset) % N_GRAPH
    within = jax.random.randint(subkeys[3], (EDGES,), 0, PEER_CAP)
    return jnp.where(is_local, local_slot, NOD_DEV + source * PEER_CAP + within).astype(jnp.int32)


def draw_send_list(key, part):
    subkeys = jax.random.split(jax.random.fold_in(key, 23), N_GRAPH * N_GRAPH)

    def one_list(row_key):
        return jax.random.permutation(row_key, NOD_DEV)[:PEER_CAP]
    return jax.vmap(one_list)(subkeys).astype(jnp.int32)


def draw_edge_count(key, part):
    subkeys = jax.random.split(jax.random.fold_in(key, 37), 2)
    counts = jax.random.randint(subkeys[0], (N_GRAPH,), EDGE_CAP // 4, EDGE_CAP + 1)
    fullest = jax.random.randint(subkeys[1], (), 0, N_GRAPH)
    return jnp.where(jnp.arange(N_GRAPH) == fullest, EDGE_CAP, counts).astype(jnp.int32)


def with_ends(array, stream_key, smallest, top_value):
    shape = array.shape
    index_at = [jax.random.randint(jax.random.fold_in(stream_key, axis), (), 0, shape[axis]) for axis in range(len(shape))]
    array = array.at[tuple(index_at)].set(smallest)
    longest = shape.index(max(shape))
    index_at[longest] = (index_at[longest] + 1) % shape[longest]
    return array.at[tuple(index_at)].set(top_value)


def shard_levels(stream_key, shape, cuts, low, largest):
    level = 1.0
    for position, blocks in cuts:
        heights = jax.random.uniform(jax.random.fold_in(jax.random.fold_in(stream_key, 6), position), (blocks,), jnp.float32, low / len(cuts), largest / len(cuts))
        level = level * jnp.repeat(jnp.exp(heights), shape[position] // blocks).reshape((-1,) + (1,) * (len(shape) - 1 - position))
    return level


def noise(own_key, shape, spread, most, cuts=(), held_as=jnp.bfloat16):
    array = spread * jax.random.normal(own_key, shape, jnp.float32)
    if cuts:
        array = array * shard_levels(own_key, shape, cuts, -0.22, 0.18)
    return jnp.clip(array, -most, most).astype(held_as)


def setup_inputs(seed: int = 0) -> dict:
    keys = jax.random.split(jax.random.key(seed), 14)
    node_latent = noise(keys[0], (SAMPLES, NODES, D), 1.0, 6.0, ((0, 4), (1, 8)))
    edge_latent = noise(keys[1], (SAMPLES, EDGES, D), 1.0, 6.0, ((0, 4), (1, 8)))
    node_cotangent = noise(keys[2], (SAMPLES, NODES, D), 1.0, 6.0, ((0, 4), (1, 8)))
    edge_w_in = noise(keys[3], (LAYERS, 3 * D, HID), (3 * D) ** -0.5, 0.15625)
    edge_w_out = noise(keys[4], (LAYERS, HID, D), HID ** -0.5, 0.25)
    node_w_in = noise(keys[5], (LAYERS, 2 * D, HID), (2 * D) ** -0.5, 0.1875)
    node_w_out = noise(keys[6], (LAYERS, HID, D), HID ** -0.5, 0.25)
    edge_gain = jnp.clip(1.0 + 0.15 * jax.random.normal(keys[7], (LAYERS, D), jnp.float32), 0.25, 1.75)
    node_gain = jnp.clip(1.0 + 0.15 * jax.random.normal(keys[8], (LAYERS, D), jnp.float32), 0.25, 1.75)
    edge_slot = draw_edge_slot(jax.random.fold_in(keys[13], 71), 0)
    edge_receiver = with_ends(jax.random.randint(keys[10], (EDGES,), 0, NOD_DEV), jax.random.fold_in(keys[10], 1), 0, NOD_DEV - 1).astype(jnp.int32)
    send_list = draw_send_list(jax.random.fold_in(keys[13], 71), 0)
    edge_count = draw_edge_count(jax.random.fold_in(keys[13], 71), 0)
    return {"node_latent": node_latent, "edge_latent": edge_latent, "node_cotangent": node_cotangent, "edge_w_in": edge_w_in, "edge_w_out": edge_w_out, "node_w_in": node_w_in, "node_w_out": node_w_out, "edge_gain": edge_gain, "node_gain": node_gain, "edge_slot": edge_slot, "edge_receiver": edge_receiver, "send_list": send_list, "edge_count": edge_count}


EPSILON = 1e-05

def mlp_forward(pieces, weights, w_out, gain, live):
    pre_act = None
    for piece, weight in zip(pieces, weights):
        term = jnp.dot(piece, weight, preferred_element_type=jnp.float32)
        pre_act = term if pre_act is None else pre_act + term
    hidden = (pre_act * jax.nn.sigmoid(pre_act)).astype(jnp.bfloat16)
    projected = jnp.dot(hidden, w_out, preferred_element_type=jnp.float32)
    centre = projected - lax.optimization_barrier(jnp.mean(projected, axis=-1, keepdims=True))
    inv_std = lax.rsqrt(lax.optimization_barrier(jnp.mean(centre * centre, axis=-1, keepdims=True)) + EPSILON)
    normed = centre * inv_std
    result = normed * gain
    if live is not None:
        result = result * live[:, None]
    return (result, (pre_act, hidden, normed, inv_std))

def mlp_backward(grad_out, pieces, weights, w_out, gain, live, saved):
    pre_act, hidden, normed, inv_std = saved
    if live is not None:
        grad_out = grad_out * live[:, None]
    grad_gain = lax.optimization_barrier(jnp.sum(grad_out * normed, axis=0))
    grad_norm = grad_out * gain
    grad_proj = inv_std * (grad_norm - lax.optimization_barrier(jnp.mean(grad_norm, axis=-1, keepdims=True)) - normed * lax.optimization_barrier(jnp.mean(grad_norm * normed, axis=-1, keepdims=True)))
    grad_proj_bf = grad_proj.astype(jnp.bfloat16)
    grad_w_out = jnp.dot(hidden.T, grad_proj_bf, preferred_element_type=jnp.float32)
    grad_hidden = jnp.dot(grad_proj_bf, w_out.T, preferred_element_type=jnp.float32)
    sigma = jax.nn.sigmoid(pre_act)
    grad_pre = grad_hidden * sigma * (1.0 + pre_act * (1.0 - sigma))
    grad_pre_bf = grad_pre.astype(jnp.bfloat16)
    grad_weights = [jnp.dot(piece.T, grad_pre_bf, preferred_element_type=jnp.float32) for piece in pieces]
    grad_pieces = [jnp.dot(grad_pre_bf, weight.T, preferred_element_type=jnp.float32) for weight in weights]
    return (grad_pieces, grad_weights, grad_w_out, grad_gain)

def run_sample(node_start, edge_start, cotangent, edge_w_in, edge_w_out, node_w_in, node_w_out, edge_gain, node_gain, sender, receiver, live):
    state = node_start.astype(jnp.float32)
    edge_state = edge_start.astype(jnp.float32)
    edge_bf = edge_start
    records = []
    for layer in range(LAYERS):
        node_bf = state.astype(jnp.bfloat16)
        if layer > 0:
            edge_bf = edge_state.astype(jnp.bfloat16)
        from_sender = node_bf[sender]
        at_receiver = node_bf[receiver]
        w_first = edge_w_in[layer]
        edge_weights = [w_first[:D], w_first[2 * D:], w_first[D:2 * D]]
        edge_inputs = [edge_bf, at_receiver, from_sender]
        message, edge_saved = mlp_forward(edge_inputs, edge_weights, edge_w_out[layer], edge_gain[layer], live)
        summed = jax.ops.segment_sum(message, receiver, num_segments=NODES).astype(jnp.bfloat16)
        n_first = node_w_in[layer]
        node_weights = [n_first[:D], n_first[D:]]
        node_inputs = [node_bf, summed]
        update, node_saved = mlp_forward(node_inputs, node_weights, node_w_out[layer], node_gain[layer], None)
        records.append((edge_inputs, edge_weights, edge_saved, node_inputs, node_weights, node_saved))
        edge_state = edge_state + message
        state = state + update
    grad_state = cotangent.astype(jnp.float32)
    grad_edge = None
    layer_grads = []
    for layer in reversed(range(LAYERS)):
        edge_inputs, edge_weights, edge_saved, node_inputs, node_weights, node_saved = records[layer]
        node_parts, node_wgrads, grad_n_out, grad_n_gain = mlp_backward(grad_state, node_inputs, node_weights, node_w_out[layer], node_gain[layer], None, node_saved)
        grad_message = node_parts[1][receiver]
        if grad_edge is not None:
            grad_message = grad_message + grad_edge
        edge_parts, edge_wgrads, grad_e_out, grad_e_gain = mlp_backward(grad_message, edge_inputs, edge_weights, edge_w_out[layer], edge_gain[layer], live, edge_saved)
        grad_edge = edge_parts[0] if grad_edge is None else edge_parts[0] + grad_edge
        grad_state = grad_state + node_parts[0] + jax.ops.segment_sum(edge_parts[1], receiver, num_segments=NODES) + jax.ops.segment_sum(edge_parts[2], sender, num_segments=NODES)
        grad_e_in = jnp.concatenate([edge_wgrads[0], edge_wgrads[2], edge_wgrads[1]], axis=0)
        grad_n_in = jnp.concatenate([node_wgrads[0], node_wgrads[1]], axis=0)
        layer_grads.append((grad_e_in, grad_e_out, grad_n_in, grad_n_out, grad_e_gain, grad_n_gain))
    layer_grads = layer_grads[::-1]
    stacked = tuple((jnp.stack([entry[index] for entry in layer_grads]) for index in range(6)))
    return (state, grad_state) + stacked

def reference(node_latent, edge_latent, node_cotangent, edge_w_in, edge_w_out, node_w_in, node_w_out, edge_gain, node_gain, edge_slot, edge_receiver, send_list, edge_count):
    edge_ids = jnp.arange(EDGES, dtype=jnp.int32)
    owner = edge_ids // EDGE_CAP
    is_local = edge_slot < NOD_DEV
    remote = jnp.where(is_local, 0, edge_slot - NOD_DEV).astype(jnp.int32)
    source = remote // PEER_CAP
    within = remote % PEER_CAP
    listed = send_list[source * N_GRAPH + owner, within]
    sender = jnp.where(is_local, owner * NOD_DEV + edge_slot, source * NOD_DEV + listed).astype(jnp.int32)
    receiver = (owner * NOD_DEV + edge_receiver).astype(jnp.int32)
    live = (edge_ids % EDGE_CAP < edge_count[owner]).astype(jnp.float32)

    def sample_fn(inputs):
        node_start, edge_start, cotangent = inputs
        return run_sample(node_start, edge_start, cotangent, edge_w_in, edge_w_out, node_w_in, node_w_out, edge_gain, node_gain, sender, receiver, live)
    results = lax.map(sample_fn, (node_latent, edge_latent, node_cotangent))
    node_out, node_grad = (results[0], results[1])
    sums = tuple((lax.optimization_barrier(jnp.sum(entry, axis=0)) for entry in results[2:]))
    return (node_out, node_grad, sums[0], sums[1], sums[2], sums[3], sums[4], sums[5])
```

```python
import functools

import jax
import jax.numpy as jnp
from jax import lax
from jax.experimental import pallas as pl
from jax.experimental.pallas import tpu as pltpu
from jax.sharding import PartitionSpec as P

EPSILON = 1e-05
BF = jnp.bfloat16
F32 = jnp.float32


def dot(a, b):
    return jnp.dot(a, b, preferred_element_type=F32)


def dot_t(a, b):
    return lax.dot_general(a, b, (((0,), (0,)), ((), ())), preferred_element_type=F32)


def dot_nt(a, b):
    return lax.dot_general(a, b, (((1,), (1,)), ((), ())), preferred_element_type=F32)


def head(pre_act, w_out, gain):
    hidden = (pre_act * jax.nn.sigmoid(pre_act)).astype(BF)
    projected = dot(hidden, w_out)
    centre = projected - jnp.mean(projected, axis=-1, keepdims=True)
    inv_std = lax.rsqrt(jnp.mean(centre * centre, axis=-1, keepdims=True) + EPSILON)
    normed = centre * inv_std
    return normed * gain, (pre_act, hidden, normed, inv_std)


def head_backward(grad_out, w_out, gain, saved):
    pre_act, hidden, normed, inv_std = saved
    grad_gain = jnp.sum(grad_out * normed, axis=0)
    grad_norm = grad_out * gain
    grad_proj = inv_std * (
        grad_norm
        - jnp.mean(grad_norm, axis=-1, keepdims=True)
        - normed * jnp.mean(grad_norm * normed, axis=-1, keepdims=True)
    )
    grad_proj_bf = grad_proj.astype(BF)
    grad_w_out = dot_t(hidden, grad_proj_bf)
    grad_hidden = dot_nt(grad_proj_bf, w_out)
    sigma = jax.nn.sigmoid(pre_act)
    grad_pre = (grad_hidden * sigma * (1.0 + pre_act * (1.0 - sigma))).astype(BF)
    return grad_pre, grad_w_out, grad_gain


def exchange(rows):
    return lax.all_to_all(rows, "graph", split_axis=0, concat_axis=0, tiled=True)


def lane_orders(groups, samples):
    batch_bits = [("batch", k) for k in range(samples.bit_length() - 1)]
    graph_bits = [("graph", k) for k in range(groups.bit_length() - 1)]
    first = batch_bits + graph_bits
    second = batch_bits[:1] + graph_bits[:1] + batch_bits[1:] + graph_bits[:0:-1]
    return first, second


def pack(terms, order, groups, samples):
    parts = groups * samples
    width = terms[0].shape[1]
    blocks = [t.astype(BF).reshape(parts, -1, width) for t in terms[:4]]
    gains = jnp.stack([t.astype(BF).reshape(parts, -1) for t in terms[4:]], axis=1)
    gains = jnp.pad(gains, ((0, 0), (0, 8 - gains.shape[1]), (0, width - gains.shape[2])))
    packed = jnp.concatenate(blocks + [gains], axis=1)
    bits = len(order)
    natural = [("graph", k) for k in range(groups.bit_length() - 1)][::-1]
    natural += [("batch", k) for k in range(samples.bit_length() - 1)][::-1]
    axes = [natural.index(bit) for bit in order]
    split = packed.reshape((2,) * bits + packed.shape[1:])
    return split.transpose(axes + [bits, bits + 1]).reshape(packed.shape)


def halving_kernel(orders, *refs):
    lanes = len(orders)
    steps = len(orders[0])
    sources, out_ref = refs[:lanes], refs[lanes]
    rest = refs[lanes + 1 :]
    landed = [rest[lane * steps : (lane + 1) * steps] for lane in range(lanes)]
    send_sem, recv_sem = rest[lanes * steps :]
    position = {"batch": lax.axis_index("batch"), "graph": lax.axis_index("graph")}

    def bit_of(axis, bit):
        return lax.rem(lax.div(position[axis], 2**bit), 2)

    def partner(axis, bit):
        return {axis: position[axis] + 2**bit * (1 - 2 * bit_of(axis, bit))}

    barrier = pltpu.get_barrier_semaphore()
    for axis, bit in orders[0]:
        pl.semaphore_signal(
            barrier, inc=1, device_id=partner(axis, bit), device_id_type=pl.DeviceIdType.MESH
        )
    pl.semaphore_wait(barrier, steps)

    def send(lane, step):
        axis, bit = orders[lane][step]
        source = sources[lane] if step == 0 else landed[lane][step - 1]
        half = source.shape[0] // 2
        copy = pltpu.make_async_remote_copy(
            src_ref=source.at[pl.ds((1 - bit_of(axis, bit)) * half, half)],
            dst_ref=landed[lane][step],
            send_sem=send_sem.at[lane * steps + step],
            recv_sem=recv_sem.at[lane * steps + step],
            device_id=partner(axis, bit),
            device_id_type=pl.DeviceIdType.MESH,
        )
        copy.start()
        return copy

    def accumulate(lane, step, start, count):
        source = sources[lane] if step == 0 else landed[lane][step - 1]
        target = landed[lane][step]
        base = bit_of(*orders[lane][step]) * target.shape[0]

        def add(i, carry):
            mine = source[base + start + i].astype(F32)
            target[start + i] = (mine + target[start + i].astype(F32)).astype(BF)
            return carry

        lax.fori_loop(0, count, add, 0)

    flying = [send(lane, 0) for lane in range(lanes)]
    started = list(flying)
    for step in range(steps):
        for lane in range(lanes):
            flying[lane].wait_recv()
            count = landed[lane][step].shape[0]
            if step + 1 < steps:
                half = count // 2
                keep = bit_of(*orders[lane][step + 1])
                accumulate(lane, step, (1 - keep) * half, half)
                flying[lane] = send(lane, step + 1)
                started.append(flying[lane])
                accumulate(lane, step, keep * half, half)
            else:
                base = bit_of(*orders[lane][step])
                last = landed[lane][step - 1]
                out_ref[lane] = last[base].astype(F32) + landed[lane][step][0].astype(F32)
    for copy in started:
        copy.wait_send()


def reduce_terms(layer_terms):
    groups = lax.axis_size("graph")
    samples = lax.axis_size("batch")
    parts = groups * samples
    choices = lane_orders(groups, samples)
    orders = [choices[i % 2] for i in range(len(layer_terms))]
    packed = [pack(t, o, groups, samples) for t, o in zip(layer_terms, orders)]
    count, per, width = packed[0].shape
    steps = len(orders[0])
    copies = len(orders) * steps
    total = pl.pallas_call(
        functools.partial(halving_kernel, orders),
        out_shape=jax.ShapeDtypeStruct((len(orders), per, width), F32),
        in_specs=[pl.BlockSpec(memory_space=pltpu.VMEM)] * len(orders),
        out_specs=pl.BlockSpec(memory_space=pltpu.VMEM),
        scratch_shapes=[
            pltpu.VMEM((count >> (step + 1), per, width), BF)
            for _ in orders
            for step in range(steps)
        ]
        + [pltpu.SemaphoreType.DMA((copies,)), pltpu.SemaphoreType.DMA((copies,))],
        compiler_params=pltpu.CompilerParams(
            collective_id=0, has_side_effects=True, vmem_limit_bytes=48 * 1024 * 1024
        ),
    )(*packed)
    out = []
    at = 0
    for t in layer_terms[0][:4]:
        rows = t.shape[0] // parts
        out.append(total[:, at : at + rows])
        at += rows
    share = layer_terms[0][4].shape[0] // parts
    out.append(total[:, at, :share])
    out.append(total[:, at + 1, :share])
    return tuple(out)


def body(
    node_latent,
    edge_latent,
    node_cotangent,
    edge_w_in,
    edge_w_out,
    node_w_in,
    node_w_out,
    edge_gain,
    node_gain,
    edge_slot,
    edge_receiver,
    send_list,
    edge_count,
):
    width = node_latent.shape[2]
    node_rows = node_latent.shape[1]
    slots = edge_slot.shape[0]
    groups = lax.axis_size("graph")
    peer_rows = send_list.shape[1]
    remote_rows = groups * peer_rows
    layers = edge_w_in.shape[0]
    live = (jnp.arange(slots, dtype=jnp.int32) < edge_count[0])[:, None]
    at_recv = (
        edge_receiver[:, None] == jnp.arange(node_rows, dtype=jnp.int32)[None, :]
    ).astype(BF)
    at_send = (
        edge_slot[:, None] == jnp.arange(node_rows + remote_rows, dtype=jnp.int32)[None, :]
    ).astype(BF)
    pick = jnp.concatenate([at_recv, at_send], axis=1)
    listed = (
        send_list.reshape(-1)[:, None] == jnp.arange(node_rows, dtype=jnp.int32)[None, :]
    ).astype(BF)
    live_f = live.astype(F32)
    state = node_latent[0].astype(F32)
    edge_state = edge_latent[0].astype(F32)
    edge_bf = edge_latent[0]
    records = []
    for layer in range(layers):
        node_bf = state.astype(BF)
        if layer > 0:
            edge_bf = edge_state.astype(BF)
        w_first = edge_w_in[layer]
        from_send = dot(node_bf, w_first[width : 2 * width]).astype(BF)
        from_recv = dot(node_bf, w_first[2 * width :]).astype(BF)
        arrived = exchange(dot(listed, from_send).astype(BF))
        table = jnp.concatenate([from_recv, from_send, arrived], axis=0)
        pre = dot(edge_bf, w_first[:width]) + dot(pick, table)
        message, edge_saved = head(pre, edge_w_out[layer], edge_gain[layer])
        message = message * live_f
        summed = dot_t(at_recv, message.astype(BF)).astype(BF)
        n_first = node_w_in[layer]
        n_pre = dot(node_bf, n_first[:width]) + dot(summed, n_first[width:])
        update, node_saved = head(n_pre, node_w_out[layer], node_gain[layer])
        records.append((edge_bf, node_bf, summed, edge_saved, node_saved))
        if layer + 1 < layers:
            edge_state = edge_state + message
        state = state + update
    grad_state = node_cotangent[0].astype(F32)
    grad_edge = None
    reduced = []
    for layer in reversed(range(layers)):
        edge_bf, node_bf, summed, edge_saved, node_saved = records[layer]
        w_first = edge_w_in[layer]
        n_first = node_w_in[layer]
        n_pre_g, grad_n_out, grad_n_gain = head_backward(
            grad_state, node_w_out[layer], node_gain[layer], node_saved
        )
        grad_state = grad_state + dot_nt(n_pre_g, n_first[:width])
        grad_sum = dot_nt(n_pre_g, n_first[width:]).astype(BF)
        grad_n_in = jnp.concatenate([dot_t(node_bf, n_pre_g), dot_t(summed, n_pre_g)], axis=0)
        grad_message = dot(at_recv, grad_sum)
        if grad_edge is not None:
            grad_message = grad_message + grad_edge
        e_pre_g, grad_e_out, grad_e_gain = head_backward(
            grad_message * live_f, edge_w_out[layer], edge_gain[layer], edge_saved
        )
        gathered = dot_t(pick, e_pre_g)
        outgoing = gathered[2 * node_rows :].astype(BF)
        arrived = exchange(outgoing)
        if layer > 0:
            part = dot_nt(e_pre_g, w_first[:width])
            grad_edge = part if grad_edge is None else part + grad_edge
        sum_recv = gathered[:node_rows].astype(BF)
        sum_send = (gathered[node_rows : 2 * node_rows] + dot_t(listed, arrived)).astype(BF)
        grad_state = (
            grad_state
            + dot_nt(sum_send, w_first[width : 2 * width])
            + dot_nt(sum_recv, w_first[2 * width :])
        )
        grad_e_in = jnp.concatenate(
            [dot_t(edge_bf, e_pre_g), dot_t(node_bf, sum_send), dot_t(node_bf, sum_recv)], axis=0
        )
        reduced.append(
            (grad_e_in, grad_e_out, grad_n_in, grad_n_out, grad_e_gain, grad_n_gain)
        )
    return (state[None], grad_state[None]) + reduce_terms(reduced[::-1])


def solution(mesh):
    node = P("batch", "graph", None)
    in_specs = (node, node, node) + (P(),) * 6 + (P("graph"), P("graph"), P("graph", None), P("graph"))
    weight = P(None, ("graph", "batch"), None)
    gain = P(None, ("graph", "batch"))
    out_specs = (node, node, weight, weight, weight, weight, gain, gain)
    return jax.shard_map(body, mesh=mesh, in_specs=in_specs, out_specs=out_specs, check_vma=False)
```
